32 devices in a mesh: dp: 8 (over z, y), tensor: 4 (over x, core).
Axes of the slice: x: 2, y: 2, z: 4, core: 2. Of those that a mesh axis runs over, the one named last changes fastest.
Arguments:
- attention: bfloat16 [4096, 4096], P('dp', 'tensor'), may hold values from -0.44921875 to 0.546875
- cotangent: bfloat16 [4096, 2048], P('dp', 'tensor'), may hold values from -0.5 to 1.5
- projection: bfloat16 [4096, 2048], P(None, 'tensor'), may hold values from -0.125 to 0.125
Outputs:
- input_grad: bfloat16 [4096, 4096], P('dp', 'tensor')
- combined: float32 [4096, 2048], P(None, 'tensor')
The draws below stay inside these ranges and needn't reach their ends.
All inputs are finite; a program needn't handle non-finite values.
Results may differ from the reference program's by a relative error of at most 0.0004.
Values may be sent and summed in bfloat16 or wider, within the bound.
No kernel may reach another device: no remote copies, remote signals or barrier semaphores. Data moves between devices by JAX's collectives and lax.ppermute only.
A program may use at most 64 MiB of HBM per device.

```python
import jax
import jax.numpy as jnp
from jax import lax

D = 2048
QD = 4096
ROWS_DEV = 512
TOKENS = 4096
N_DP = 8


def steps_of(stream_key, extent, shards, least, high):
    def one(position, shards_of):
        draws = jax.random.uniform(jax.random.fold_in(jax.random.fold_in(stream_key, 6), position), (shards_of,), jnp.float32, least / len(shards), high / len(shards))
        return jnp.repeat(jnp.exp(draws), extent[position] // shards_of).reshape((-1,) + (1,) * (len(extent) - position - 1))

    gain = one(*shards[0])
    for cut in shards[1:]:
        gain = gain * one(*cut)
    return gain


def bell_draw(stream_key, extent, deviation, most, shards=(), kind=jnp.bfloat16):
    result = deviation * jax.random.normal(stream_key, extent, jnp.float32)
    if shards:
        result = result * steps_of(stream_key, extent, shards, -0.22, 0.18)
    return jnp.clip(result, -most, most).astype(kind)


def setup_inputs(seed: int = 0) -> dict:
    splits = jax.random.split(jax.random.key(seed), 4)
    return {
        "attention": jnp.clip(-0.44921875 + 0.99609375 * jax.random.uniform(splits[0], (TOKENS, QD), jnp.float32) ** steps_of(splits[0], (TOKENS, QD), ((0, 8), (1, 4)), -0.2, 0.2), -0.44921875, 0.546875).astype(jnp.bfloat16),
        "cotangent": jnp.clip(-0.5 + 2.0 * jax.random.uniform(splits[1], (TOKENS, D), jnp.float32) ** steps_of(splits[1], (TOKENS, D), ((0, 8), (1, 4)), -0.2, 0.2), -0.5, 1.5).astype(jnp.bfloat16),
        "projection": bell_draw(splits[2], (QD, D), D ** -0.5, 0.125, ((1, 4),)),
    }


epsilon = 1e-06

def pair_merge(lower_vec, upper_vec):
    lower_sq = jnp.sum(lower_vec * lower_vec) + epsilon
    upper_sq = jnp.sum(upper_vec * upper_vec) + epsilon
    cross = jnp.sum(lower_vec * upper_vec)
    return (1.0 - cross / (2.0 * lower_sq)) * lower_vec + (1.0 - cross / (2.0 * upper_sq)) * upper_vec

def replica_grad(attention, cotangent, replica):
    row_start = replica * ROWS_DEV
    acts_rows = attention[row_start:row_start + ROWS_DEV]
    cot_rows = cotangent[row_start:row_start + ROWS_DEV]
    return jnp.dot(acts_rows.T, cot_rows, preferred_element_type=jnp.float32)

def tree_merge(attention, cotangent, first_index, span_size):
    if span_size == 1:
        return replica_grad(attention, cotangent, first_index)
    half_span = span_size // 2
    lower_vec = tree_merge(attention, cotangent, first_index, half_span)
    upper_vec = tree_merge(attention, cotangent, first_index + half_span, half_span)
    return pair_merge(lower_vec, upper_vec)

def reference(attention, cotangent, projection):

    def input_block(cot_rows):
        return jnp.dot(cot_rows, projection.T, preferred_element_type=jnp.float32).astype(jnp.bfloat16)
    blocks = lax.map(input_block, cotangent.reshape(N_DP, ROWS_DEV, D))
    input_grad = blocks.reshape(N_DP * ROWS_DEV, QD)
    combined = tree_merge(attention, cotangent, 0, N_DP)
    return (input_grad, combined)
```

```python
import jax
import jax.numpy as jnp
from jax import lax
from jax.sharding import PartitionSpec as P

epsilon = 1e-06


def merge_coefs(gram):
    n = gram.shape[0]
    coefs = [jnp.zeros((n,), jnp.float32).at[i].set(1.0) for i in range(n)]
    while len(coefs) > 1:
        merged = []
        for low, high in zip(coefs[0::2], coefs[1::2]):
            low_g = jnp.sum(gram * low[:, None], 0)
            high_g = jnp.sum(gram * high[:, None], 0)
            low_sq = jnp.maximum(jnp.sum(low_g * low), 0.0)
            high_sq = jnp.maximum(jnp.sum(high_g * high), 0.0)
            most = jnp.sqrt(low_sq) * jnp.sqrt(high_sq)
            cross = jnp.clip(jnp.sum(low_g * high), -most, most)
            merged.append(
                (1.0 - cross / (2.0 * (low_sq + epsilon))) * low
                + (1.0 - cross / (2.0 * (high_sq + epsilon))) * high
            )
        coefs = merged
    return coefs[0]


def on_device(attention, cotangent, projection):
    n, groups = lax.axis_size("dp"), lax.axis_size("tensor")
    rows = attention.shape[0]
    own_rows = lax.all_to_all(projection, "tensor", split_axis=0, concat_axis=1, tiled=True)
    input_grad = lax.dot_general(
        lax.all_gather(cotangent, "tensor", axis=1, tiled=True),
        own_rows,
        (((1,), (1,)), ((), ())),
        preferred_element_type=jnp.float32,
    ).astype(jnp.bfloat16)

    acts = lax.all_to_all(attention, "dp", split_axis=1, concat_axis=0, tiled=True)
    acts = lax.all_gather(acts, "tensor", axis=1, tiled=True)
    cots = lax.all_gather(cotangent, "dp", axis=0, tiled=True)
    features, columns = acts.shape[1], cots.shape[1]
    grads = [
        lax.dot_general(
            acts[s * rows : (s + 1) * rows],
            cots[s * rows : (s + 1) * rows],
            (((0,), (0,)), ((), ())),
            preferred_element_type=jnp.float32,
        )
        for s in range(n)
    ]
    gram = jnp.stack([jnp.stack([jnp.sum(grads[i] * grads[j]) for j in range(n)]) for i in range(n)])
    gram = lax.psum(gram, ("dp", "tensor"))
    coefs = merge_coefs(gram)
    bound = jnp.sum(jnp.abs(coefs) * jnp.sqrt(jnp.diagonal(gram)))
    scale = jnp.exp2(jnp.floor(jnp.log2(jnp.maximum(bound, 1e-30)))+1)
    piece = sum(coefs[s] * grads[s] for s in range(n))
    sent = (piece * (16384.0 / scale)).astype(jnp.float16)
    gathered = lax.all_gather(sent, "dp", axis=0)
    combined = gathered.astype(jnp.float32) * (scale / 16384.0)
    combined = combined.reshape(n, groups, features // groups, columns).transpose(1, 0, 2, 3).reshape(-1, columns)
    return (input_grad, combined)


def solution(mesh):
    return jax.shard_map(
        on_device,
        mesh=mesh,
        in_specs=(P("dp", "tensor"), P("dp", "tensor"), P(None, "tensor")),
        out_specs=(P("dp", "tensor"), P(None, "tensor")),
        check_vma=False,
    )
```

```python
import functools

import jax
import jax.numpy as jnp
from jax import lax
from jax.experimental import pallas as pl
from jax.experimental.pallas import tpu as pltpu
from jax.sharding import PartitionSpec as P

epsilon = 1e-06
tiny = 1e-30
peak = 16384.0
lanes = 128


def pair_weights(low_sq, high_sq, cross):
    low_sq = jnp.maximum(low_sq, 0.0)
    high_sq = jnp.maximum(high_sq, 0.0)
    most = jnp.sqrt(low_sq) * jnp.sqrt(high_sq)
    cross = jnp.minimum(jnp.maximum(cross, -most), most)
    return 1.0 - cross / (2.0 * (low_sq + epsilon)), 1.0 - cross / (2.0 * (high_sq + epsilon))


def merge_coefs(products):
    count = len(products)
    members = [{i: None} for i in range(count)]
    table = products
    while len(table) > 1:
        half = len(table) // 2
        weights = [
            pair_weights(table[2 * i][2 * i], table[2 * i + 1][2 * i + 1], table[2 * i][2 * i + 1])
            for i in range(half)
        ]
        members = [
            {
                r: weights[i][side] if w is None else weights[i][side] * w
                for side in (0, 1)
                for r, w in members[2 * i + side].items()
            }
            for i in range(half)
        ]
        table = [
            [
                sum(
                    weights[i][a] * weights[j][b] * table[min(2 * i + a, 2 * j + b)][max(2 * i + a, 2 * j + b)]
                    for a in (0, 1)
                    for b in (0, 1)
                )
                if j >= i
                else None
                for j in range(half)
            ]
            for i in range(half)
        ]
    return [members[0][r] for r in range(count)]


def own_input_grad(cotangent, projection):
    own_rows = lax.all_to_all(projection, "tensor", split_axis=0, concat_axis=1, tiled=True)
    return lax.dot_general(
        lax.all_gather(cotangent, "tensor", axis=1, tiled=True),
        own_rows,
        (((1,), (1,)), ((), ())),
        preferred_element_type=jnp.float32,
    ).astype(jnp.bfloat16)


def whole_gathers(attention, cotangent, projection):
    n, groups = lax.axis_size("dp"), lax.axis_size("tensor")
    rows = attention.shape[0]
    input_grad = own_input_grad(cotangent, projection)
    acts = lax.all_to_all(attention, "dp", split_axis=1, concat_axis=0, tiled=True)
    acts = lax.all_gather(acts, "tensor", axis=1, tiled=True)
    cots = lax.all_gather(cotangent, "dp", axis=0, tiled=True)
    features, columns = acts.shape[1], cots.shape[1]
    grads = lax.dot_general(
        acts.reshape(n, rows, features),
        cots.reshape(n, rows, columns),
        (((1,), (1,)), ((0,), (0,))),
        preferred_element_type=jnp.float32,
    )
    gram = jnp.stack([jnp.sum(grads * grads[i], (1, 2)) for i in range(n)])
    gram = lax.psum(gram, ("dp", "tensor"))
    coefs = jnp.stack(merge_coefs([[gram[i, j] for j in range(n)] for i in range(n)]))
    bound = jnp.maximum(jnp.sum(jnp.abs(coefs) * jnp.sqrt(jnp.diagonal(gram))), tiny)
    piece = jnp.sum(coefs[:, None, None] * grads, 0)
    sent = (piece * (peak / bound)).astype(jnp.float16)
    gathered = lax.all_gather(sent, "dp", axis=0).astype(jnp.float32) * (bound / peak)
    gathered = gathered.reshape(n, groups, features // groups, columns)
    return (input_grad, gathered.transpose(1, 0, 2, 3).reshape(-1, columns))


def grads_kernel(steps, replicas, slots, before, index_ref, *refs):
    slices = refs[: len(slots)]
    cots = refs[len(slots) : len(slots) + replicas]
    earlier = refs[len(slots) + replicas : -2]
    grads_ref, gram_ref = refs[-2:]
    width = slices[0].shape[2]
    for l in range(replicas):
        for m, piece in enumerate(slices):
            at = pl.multiple_of(index_ref[steps + m] * width, width)
            grads_ref[l, pl.ds(at, width), :] = lax.dot_general(
                piece[l],
                cots[l][...],
                (((0,), (0,)), ((), ())),
                preferred_element_type=jnp.float32,
            )
    blocks = [(ref, l) for ref in earlier for l in range(replicas)] + [(grads_ref, l) for l in range(replicas)]
    pairs = [(a, b) for b in range(before, before + replicas) for a in range(b + 1)]
    features, columns = grads_ref.shape[1:]

    def body(chunk, sums):
        at = pl.multiple_of(chunk * 8, 8)
        values = [ref[l, pl.ds(at, 8), :] for ref, l in blocks]
        fresh = []
        for (a, b), total in zip(pairs, sums):
            product = values[a] * values[b]
            for j in range(columns // lanes):
                total = total + product[:, j * lanes : (j + 1) * lanes]
            fresh.append(total)
        return tuple(fresh)

    zero = jnp.zeros((8, lanes), jnp.float32)
    sums = lax.fori_loop(0, features // 8, body, tuple(zero for _ in pairs))
    row = lax.broadcasted_iota(jnp.int32, (8, lanes), 0)
    col = lax.broadcasted_iota(jnp.int32, (8, lanes), 1)
    gram = zero
    for (a, b), total in zip(pairs, sums):
        value = jnp.sum(jnp.sum(total, axis=0, keepdims=True), axis=1, keepdims=True)
        low = jnp.minimum(index_ref[a], index_ref[b])
        high = jnp.maximum(index_ref[a], index_ref[b])
        gram = gram + jnp.where((row == low) & (col == high), value, 0.0)
    gram_ref[...] = gram


def combine_kernel(replicas, index_ref, gram_ref, *refs):
    blocks, (piece_ref, scale_ref) = refs[:-2], refs[-2:]
    count = len(blocks) * replicas
    gram = jnp.sum(gram_ref[...], axis=0)
    row = lax.broadcasted_iota(jnp.int32, gram.shape, 0)
    col = lax.broadcasted_iota(jnp.int32, gram.shape, 1)

    def entry(i, j):
        found = jnp.where((row == i) & (col == j), gram, 0.0)
        return jnp.sum(jnp.sum(found, axis=0, keepdims=True), axis=1, keepdims=True)

    products = [[entry(i, j) if j >= i else None for j in range(count)] for i in range(count)]
    coefs = merge_coefs(products)
    bound = sum(jnp.abs(coefs[i]) * jnp.sqrt(products[i][i]) for i in range(count))
    bound = jnp.maximum(bound, tiny)
    by_replica = sum(jnp.where(col[:1] == i, coefs[i], 0.0) for i in range(count))
    weights = []
    for at in range(count):
        mine = jnp.where(col[:1] == index_ref[at], by_replica, 0.0)
        weights.append(jnp.sum(mine, axis=1, keepdims=True) * (peak / bound))
    features, columns = piece_ref.shape

    def body(chunk, carry):
        at = pl.multiple_of(chunk * 16, 16)
        total = None
        for block in range(len(blocks)):
            for l in range(replicas):
                term = blocks[block][l, pl.ds(at, 16), :] * weights[block * replicas + l]
                total = term if total is None else total + term
        piece_ref[pl.ds(at, 16), :] = total
        return carry

    lax.fori_loop(0, features // 16, body, 0)
    scale_ref[...] = jnp.broadcast_to(bound * (1.0 / peak), scale_ref.shape)


def in_vmem(count):
    return [pl.BlockSpec(memory_space=pltpu.VMEM)] * count


def exchanges(attention, cotangent, projection):
    n, groups = lax.axis_size("dp"), lax.axis_size("tensor")
    inner = 2 ** ((n.bit_length() - 1) // 2)
    outer, pairs = n // inner, groups // 2
    rows, features_here = attention.shape
    columns = cotangent.shape[1]
    width = features_here // n
    features = width * groups
    me, part = lax.axis_index("dp"), lax.axis_index("tensor")
    z, y = me // inner, me % inner
    x, core = part // 2, part % 2

    def along_z(value, k):
        ring = [(i * inner + j, (i + k) % outer * inner + j) for i in range(outer) for j in range(inner)]
        return lax.ppermute(value, "dp", ring)

    def along_y(value, l):
        ring = [(i * inner + j, i * inner + (j + l) % inner) for i in range(outer) for j in range(inner)]
        return lax.ppermute(value, "dp", ring)

    def along_tensor(value, j, flip):
        ring = [(a * 2 + c, (a + j) % pairs * 2 + (c ^ flip)) for a in range(pairs) for c in range(2)]
        return lax.ppermute(value, "tensor", ring)

    def gather_lines(value):
        found = {0: value}
        right = outer // 2
        for k in range(1, right + 1):
            found[k] = along_z(found[k - 1], 1)
            if outer - k > right:
                found[outer - k] = along_z(found[(outer - k + 1) % outer], -1)
        return [[found[k]] + [along_y(found[k], l) for l in range(1, inner)] for k in range(outer)]

    by_target = attention.reshape(rows, outer, inner, width).transpose(2, 1, 0, 3)
    by_y = [
        lax.dynamic_index_in_dim(by_target, (y + l) % inner, 0, keepdims=False) for l in range(inner)
    ]
    from_y = [by_y[0]] + [along_y(by_y[l], l) for l in range(1, inner)]
    from_y = jnp.stack(from_y)
    slices, slots = [], []
    for k in range(outer):
        outgoing = lax.dynamic_index_in_dim(from_y, (z + k) % outer, 1, keepdims=False)
        held = along_z(outgoing, k) if k else outgoing
        shifted = [held] + [along_tensor(held, j, 0) for j in range(1, pairs)]
        slices.append(shifted + [along_tensor(value, 0, 1) for value in shifted])
    for flip in (0, 1):
        slots += [(x - j) % pairs * 2 + (core ^ flip) for j in range(pairs)]

    cots = gather_lines(cotangent)
    replica_of = [
        [(z - k) % outer * inner + (y - l) % inner for l in range(inner)] for k in range(outer)
    ]
    order = [r for line in replica_of for r in line]
    index = jnp.stack([jnp.asarray(v, jnp.int32) for v in order + slots])
    grads, gram = [], None
    for k in range(outer):
        block, partial = pl.pallas_call(
            functools.partial(grads_kernel, n, inner, slots, k * inner),
            out_shape=(
                jax.ShapeDtypeStruct((inner, features, columns), jnp.float32),
                jax.ShapeDtypeStruct((8, lanes), jnp.float32),
            ),
            in_specs=[pl.BlockSpec(memory_space=pltpu.SMEM)] + in_vmem(groups + inner + k),
            out_specs=tuple(in_vmem(2)),
            cost_estimate=pl.CostEstimate(
                flops=2 * inner * rows * features * columns,
                bytes_accessed=8 * inner * features * columns,
                transcendentals=0,
            ),
            name=f"grads_{k}",
        )(index, *slices[k], *cots[k], *grads)
        grads.append(block)
        gram = partial if gram is None else gram + partial

    shared = lax.all_to_all(
        jnp.broadcast_to(gram[None], (n * groups, 8, lanes)), ("dp", "tensor"), 0, 0, tiled=True
    ).reshape(n * groups, 8, lanes)
    piece, scale = pl.pallas_call(
        functools.partial(combine_kernel, inner),
        out_shape=(
            jax.ShapeDtypeStruct((features, columns), jnp.float32),
            jax.ShapeDtypeStruct((8, lanes), jnp.float32),
        ),
        in_specs=[pl.BlockSpec(memory_space=pltpu.SMEM)] + in_vmem(1 + outer),
        out_specs=tuple(in_vmem(2)),
        cost_estimate=pl.CostEstimate(
            flops=2 * n * features * columns, bytes_accessed=4 * n * features * columns, transcendentals=0
        ),
        name="combine",
    )(index, shared, *grads)
    sent = piece.astype(jnp.float16)
    scale = scale[0, 0]
    combined = jnp.zeros((groups, n, width, columns), jnp.float32)
    for k, line in enumerate(gather_lines(sent)):
        for l, block in enumerate(line):
            values = block.reshape(groups, 1, width, columns).astype(jnp.float32) * scale
            combined = lax.dynamic_update_slice_in_dim(combined, values, replica_of[k][l], 1)
    combined = combined.reshape(groups * n * width, columns)

    own_cots, own_rows = lax.optimization_barrier((cotangent, projection, gram))[:2]
    own_rows = own_rows.reshape(groups, -1, columns)
    total = None
    line = [own_cots] + [along_tensor(own_cots, j, 0) for j in range(1, pairs)]
    for flip in (0, 1):
        for j in range(pairs):
            target = (x + j) % pairs * 2 + (core ^ flip)
            block = lax.dynamic_index_in_dim(own_rows, target, 0, keepdims=False)
            theirs = line[j]
            if j or flip:
                block = along_tensor(block, j, flip)
            if flip:
                theirs = along_tensor(theirs, 0, 1)
            term = lax.dot_general(
                theirs, block, (((1,), (1,)), ((), ())), preferred_element_type=jnp.float32
            )
            total = term if total is None else total + term
    return (total.astype(jnp.bfloat16), combined)


def on_device(attention, cotangent, projection):
    n, groups = lax.axis_size("dp"), lax.axis_size("tensor")
    aligned = (attention.shape[1] // n) % lanes == 0 and cotangent.shape[1] % lanes == 0
    if aligned and groups % 2 == 0 and 4 <= n <= 8:
        return exchanges(attention, cotangent, projection)
    return whole_gathers(attention, cotangent, projection)


def solution(mesh):
    return jax.shard_map(
        on_device,
        mesh=mesh,
        in_specs=(P("dp", "tensor"), P("dp", "tensor"), P(None, "tensor")),
        out_specs=(P("dp", "tensor"), P(None, "tensor")),
        check_vma=False,
    )
```

```python
import functools

import jax
import jax.numpy as jnp
from jax import lax
from jax.experimental import pallas as pl
from jax.experimental.pallas import tpu as pltpu
from jax.sharding import PartitionSpec as P


epsilon = 1e-06
tiny = 1e-30
peak = 16384.0
lanes = 128


def pair_weights(low_sq, high_sq, cross):
    low_sq = jnp.maximum(low_sq, 0.0)
    high_sq = jnp.maximum(high_sq, 0.0)
    most = jnp.sqrt(low_sq) * jnp.sqrt(high_sq)
    cross = jnp.minimum(jnp.maximum(cross, -most), most)
    return 1.0 - cross / (2.0 * (low_sq + epsilon)), 1.0 - cross / (2.0 * (high_sq + epsilon))


def merge_coefs(products):
    count = len(products)
    members = [{i: None} for i in range(count)]
    table = products
    while len(table) > 1:
        half = len(table) // 2
        weights = [
            pair_weights(table[2 * i][2 * i], table[2 * i + 1][2 * i + 1], table[2 * i][2 * i + 1])
            for i in range(half)
        ]
        members = [
            {
                r: weights[i][side] if w is None else weights[i][side] * w
                for side in (0, 1)
                for r, w in members[2 * i + side].items()
            }
            for i in range(half)
        ]
        table = [
            [
                sum(
                    weights[i][a] * weights[j][b] * table[min(2 * i + a, 2 * j + b)][max(2 * i + a, 2 * j + b)]
                    for a in (0, 1)
                    for b in (0, 1)
                )
                if j >= i
                else None
                for j in range(half)
            ]
            for i in range(half)
        ]
    return [members[0][r] for r in range(count)]


def own_input_grad(cotangent, projection):
    own_rows = lax.all_to_all(projection, "tensor", split_axis=0, concat_axis=1, tiled=True)
    return lax.dot_general(
        lax.all_gather(cotangent, "tensor", axis=1, tiled=True),
        own_rows,
        (((1,), (1,)), ((), ())),
        preferred_element_type=jnp.float32,
    ).astype(jnp.bfloat16)


def whole_gathers(attention, cotangent, projection):
    n, groups = lax.axis_size("dp"), lax.axis_size("tensor")
    rows = attention.shape[0]
    input_grad = own_input_grad(cotangent, projection)
    acts = lax.all_to_all(attention, "dp", split_axis=1, concat_axis=0, tiled=True)
    acts = lax.all_gather(acts, "tensor", axis=1, tiled=True)
    cots = lax.all_gather(cotangent, "dp", axis=0, tiled=True)
    features, columns = acts.shape[1], cots.shape[1]
    grads = lax.dot_general(
        acts.reshape(n, rows, features),
        cots.reshape(n, rows, columns),
        (((1,), (1,)), ((0,), (0,))),
        preferred_element_type=jnp.float32,
    )
    gram = jnp.stack([jnp.sum(grads * grads[i], (1, 2)) for i in range(n)])
    gram = lax.psum(gram, ("dp", "tensor"))
    coefs = jnp.stack(merge_coefs([[gram[i, j] for j in range(n)] for i in range(n)]))
    bound = jnp.maximum(jnp.sum(jnp.abs(coefs) * jnp.sqrt(jnp.diagonal(gram))), tiny)
    piece = jnp.sum(coefs[:, None, None] * grads, 0)
    sent = (piece * (peak / bound)).astype(jnp.float16)
    gathered = lax.all_gather(sent, "dp", axis=0).astype(jnp.float32) * (bound / peak)
    gathered = gathered.reshape(n, groups, features // groups, columns)
    return (input_grad, gathered.transpose(1, 0, 2, 3).reshape(-1, columns))


def fetch(pairs, sems):
    copies = [pltpu.make_async_copy(source, target, sems.at[i]) for i, (source, target) in enumerate(pairs)]
    for copy in copies:
        copy.start()
    return copies


def grads_kernel(replicas, groups, before, index_ref, *refs):
    slices, refs = refs[:groups], refs[groups:]
    cots, refs = refs[:replicas], refs[replicas:]
    earlier, refs = refs[: before // replicas], refs[before // replicas :]
    grads_ref, gram_ref, acts, cotangents, held, sems = refs
    width, columns = acts.shape[3], cotangents.shape[2]
    lines = len(earlier)
    features = groups * width
    loads = fetch(
        [(slices[m], acts.at[m]) for m in range(groups)]
        + [(cots[l], cotangents.at[l]) for l in range(replicas)]
        + [(earlier[i], held.at[i]) for i in range(lines)],
        sems,
    )
    for copy in loads[: groups + replicas]:
        copy.wait()
    for l in range(replicas):
        for m in range(groups):
            at = pl.multiple_of(index_ref[m] * width, width)
            held[lines, l, pl.ds(at, width), :] = lax.dot_general(
                acts[m, l],
                cotangents[l],
                (((0,), (0,)), ((), ())),
                preferred_element_type=jnp.float32,
            )
    store = pltpu.make_async_copy(held.at[lines], grads_ref, sems.at[len(loads)])
    store.start()
    for copy in loads[groups + replicas :]:
        copy.wait()
    blocks = [(i, l) for i in range(lines + 1) for l in range(replicas)]
    pairs = [(a, b) for b in range(before, before + replicas) for a in range(b + 1)]

    def body(chunk, sums):
        at = pl.multiple_of(chunk * 8, 8)
        values = [held[i, l, pl.ds(at, 8), :] for i, l in blocks]
        fresh = []
        for (a, b), total in zip(pairs, sums):
            product = values[a] * values[b]
            for j in range(columns // lanes):
                total = total + product[:, j * lanes : (j + 1) * lanes]
            fresh.append(total)
        return tuple(fresh)

    zero = jnp.zeros((8, lanes), jnp.float32)
    sums = lax.fori_loop(0, features // 8, body, tuple(zero for _ in pairs))
    row = lax.broadcasted_iota(jnp.int32, (8, lanes), 0)
    col = lax.broadcasted_iota(jnp.int32, (8, lanes), 1)
    gram = zero
    for (a, b), total in zip(pairs, sums):
        value = jnp.sum(jnp.sum(total, axis=0, keepdims=True), axis=1, keepdims=True)
        low = jnp.minimum(index_ref[groups + a], index_ref[groups + b])
        high = jnp.maximum(index_ref[groups + a], index_ref[groups + b])
        gram = gram + jnp.where((row == low) & (col == high), value, 0.0)
    gram_ref[...] = gram
    store.wait()


def combine_kernel(replicas, groups, index_ref, gram_ref, *refs):
    blocks, (piece_ref, scale_ref, held, sems) = refs[:-4], refs[-4:]
    count = len(blocks) * replicas
    loads = fetch([(block, held.at[i]) for i, block in enumerate(blocks)], sems)
    gram = jnp.sum(gram_ref[...], axis=0)
    row = lax.broadcasted_iota(jnp.int32, gram.shape, 0)
    col = lax.broadcasted_iota(jnp.int32, gram.shape, 1)

    def entry(i, j):
        found = jnp.where((row == i) & (col == j), gram, 0.0)
        return jnp.sum(jnp.sum(found, axis=0, keepdims=True), axis=1, keepdims=True)

    products = [[entry(i, j) if j >= i else None for j in range(count)] for i in range(count)]
    coefs = merge_coefs(products)
    bound = sum(jnp.abs(coefs[i]) * jnp.sqrt(products[i][i]) for i in range(count))
    bound = jnp.maximum(bound, tiny)
    scale_ref[...] = bound * (1.0 / peak)
    weights = []
    for at in range(count):
        weight = sum(jnp.where(index_ref[groups + at] == i, coefs[i], 0.0) for i in range(count))
        weights.append(weight * (peak / bound))
    features, _ = piece_ref.shape
    for copy in loads:
        copy.wait()

    def body(chunk, carry):
        at = pl.multiple_of(chunk * 16, 16)
        total = None
        for block in range(len(blocks)):
            for l in range(replicas):
                term = held[block, l, pl.ds(at, 16), :] * weights[block * replicas + l]
                total = term if total is None else total + term
        piece_ref[pl.ds(at, 16), :] = total
        return carry

    lax.fori_loop(0, features // 16, body, 0)


def pack_kernel(index_ref, attention_ref, packed_ref):
    packed_ref[...] = attention_ref[...].reshape(packed_ref.shape)


def pack(index, attention, width):
    rows = attention.shape[0]
    return pl.pallas_call(
        pack_kernel,
        grid_spec=pltpu.PrefetchScalarGridSpec(
            num_scalar_prefetch=1,
            grid=(index.shape[0],),
            in_specs=[pl.BlockSpec((rows, width), lambda i, index: (0, index[i]))],
            out_specs=pl.BlockSpec((1, rows, width), lambda i, index: (i, 0, 0)),
        ),
        out_shape=jax.ShapeDtypeStruct((index.shape[0], rows, width), attention.dtype),
        compiler_params=pltpu.CompilerParams(vmem_limit_bytes=4 * 2**20),
        name="pack",
    )(index, attention)


def after(value, *others):
    return lax.optimization_barrier((value, *others))[0]


def unwritten(shape):
    return pl.pallas_call(
        lambda out_ref: None,
        out_shape=jax.ShapeDtypeStruct(shape, jnp.float32),
        out_specs=pl.BlockSpec(memory_space=pltpu.HBM),
        name="unwritten",
    )()


def exchanges(attention, cotangent, projection):
    n, groups = lax.axis_size("dp"), lax.axis_size("tensor")
    inner = 2 ** ((n.bit_length() - 1) // 2)
    outer, pairs = n // inner, groups // 2
    rows, features_here = attention.shape
    columns = cotangent.shape[1]
    width = features_here // n
    features = width * groups
    me, part = lax.axis_index("dp"), lax.axis_index("tensor")
    z, y = me // inner, me % inner
    x, core = part // 2, part % 2

    def along_z(value, k):
        ring = [(i * inner + j, (i + k) % outer * inner + j) for i in range(outer) for j in range(inner)]
        return lax.ppermute(value, "dp", ring)

    def along_y(value, l):
        ring = [(i * inner + j, i * inner + (j + l) % inner) for i in range(outer) for j in range(inner)]
        return lax.ppermute(value, "dp", ring)

    def along_tensor(value, j, flip):
        ring = [(a * 2 + c, (a + j) % pairs * 2 + (c ^ flip)) for a in range(pairs) for c in range(2)]
        return lax.ppermute(value, "tensor", ring)

    right = outer // 2
    arrival = [0, 1]
    for k in range(1, right + 1):
        arrival += [outer - k] if outer - k > right else []
        arrival += [k + 1] if k < right else []

    def gather_lines(value):
        found = {0: value}
        for k in arrival[1:]:
            source, step = (found[(k + 1) % outer], -1) if k > right else (found[k - 1], 1)
            found[k] = along_z(source, step)
        return {k: [found[k]] + [along_y(found[k], l) for l in range(1, inner)] for k in arrival}

    def replica_of(k, l):
        return (z - k) % outer * inner + (y - l) % inner

    cots = gather_lines(cotangent)

    own_rows = projection.reshape(groups, -1, columns)

    def rows_for(j, flip):
        target = (x + j) % pairs * 2 + (core ^ flip)
        return lax.dynamic_index_in_dim(own_rows, target, 0, keepdims=False)

    row_blocks = {
        (j, flip): along_tensor(rows_for(j, flip), j, flip) if j or flip else rows_for(0, 0)
        for j in range(pairs)
        for flip in (0, 1)
    }
    cot_blocks = {(j, 0): along_tensor(cotangent, j, 0) if j else cotangent for j in range(pairs)}
    cot_blocks.update({(j, 1): along_tensor(cot_blocks[j, 0], 0, 1) for j in range(pairs)})

    targets = [
        jnp.stack([(z + k) % outer * inner + (y + l) % inner for k in range(outer)]).astype(jnp.int32)
        for l in range(inner)
    ]
    from_y = [
        along_y(pack(targets[l], attention, width), l) if l else pack(targets[0], attention, width)
        for l in range(inner)
    ]
    slices, slots = {}, []
    for k in arrival:
        held = jnp.stack([from_y[l][k] for l in range(inner)])
        if k:
            held = along_z(held, k)
        shifted = [held] + [along_tensor(held, j, 0) for j in range(1, pairs)]
        slices[k] = shifted + [along_tensor(value, 0, 1) for value in shifted]
    for flip in (0, 1):
        slots += [(x - j) % pairs * 2 + (core ^ flip) for j in range(pairs)]

    order = [replica_of(k, l) for k in arrival for l in range(inner)]
    index = jnp.stack([jnp.asarray(v, jnp.int32) for v in slots + order])
    grads, gram = [], None
    smem, hbm = pl.BlockSpec(memory_space=pltpu.SMEM), pl.BlockSpec(memory_space=pltpu.HBM)
    for at, k in enumerate(arrival):
        operands = [*slices[k], *cots[k], *grads]
        block, partial = pl.pallas_call(
            functools.partial(grads_kernel, inner, groups, at * inner),
            in_specs=[smem] + [hbm] * len(operands),
            out_specs=(hbm, pl.BlockSpec(memory_space=pltpu.VMEM)),
            out_shape=(
                jax.ShapeDtypeStruct((inner, features, columns), jnp.float32),
                jax.ShapeDtypeStruct((8, lanes), jnp.float32),
            ),
            scratch_shapes=[
                pltpu.VMEM((groups, inner, rows, width), attention.dtype),
                pltpu.VMEM((inner, rows, columns), cotangent.dtype),
                pltpu.VMEM((at + 1, inner, features, columns), jnp.float32),
                pltpu.SemaphoreType.DMA((len(operands) + 1,)),
            ],
            cost_estimate=pl.CostEstimate(
                flops=2 * inner * rows * features * columns,
                bytes_accessed=8 * inner * features * columns,
                transcendentals=0,
            ),
        )(index, *operands)
        grads.append(block)
        gram = partial if gram is None else gram + partial

    shared = lax.all_to_all(
        jnp.broadcast_to(gram[None], (n * groups, 8, lanes)), ("dp", "tensor"), 0, 0, tiled=True
    ).reshape(n * groups, 8, lanes)
    sent, scale = pl.pallas_call(
        functools.partial(combine_kernel, inner, groups),
        in_specs=[smem, pl.BlockSpec(memory_space=pltpu.VMEM)] + [hbm] * outer,
        out_specs=(pl.BlockSpec(memory_space=pltpu.VMEM), pl.BlockSpec(memory_space=pltpu.VMEM)),
        out_shape=(
            jax.ShapeDtypeStruct((features, columns), jnp.float32),
            jax.ShapeDtypeStruct((1, 1), jnp.float32),
        ),
        scratch_shapes=[
            pltpu.VMEM((outer, inner, features, columns), jnp.float32),
            pltpu.SemaphoreType.DMA((outer,)),
        ],
        cost_estimate=pl.CostEstimate(
            flops=2 * n * features * columns, bytes_accessed=4 * n * features * columns, transcendentals=0
        ),
        name="combine",
    )(index, shared, *grads)
    combined = unwritten((groups, n, width, columns))
    lines = gather_lines(after(sent.astype(jnp.float16)))
    for l in range(inner):
        for k in arrival:
            values = lines[k][l].reshape(groups, 1, width, columns).astype(jnp.float32) * scale[0, 0]
            combined = lax.dynamic_update_slice_in_dim(combined, values, replica_of(k, l), 1)
    combined = combined.reshape(groups * n * width, columns)

    total = None
    for key in [(0, 0), (0, 1)] + [(j, flip) for j in range(1, pairs) for flip in (0, 1)]:
        theirs = cot_blocks[key]
        if key != (0, 0):
            theirs = after(theirs, lines[outer - 1 if key[0] else 1][0])
        term = lax.dot_general(theirs, row_blocks[key], (((1,), (1,)), ((), ())), preferred_element_type=jnp.float32)
        total = term if total is None else total + term
    return (total.astype(jnp.bfloat16), combined)


def on_device(attention, cotangent, projection):
    n, groups = lax.axis_size("dp"), lax.axis_size("tensor")
    aligned = (attention.shape[1] // n) % lanes == 0 and cotangent.shape[1] % lanes == 0
    if aligned and groups % 2 == 0 and 4 <= n <= 8:
        return exchanges(attention, cotangent, projection)
    return whole_gathers(attention, cotangent, projection)


def solution(mesh):
    return jax.shard_map(
        on_device,
        mesh=mesh,
        in_specs=(P("dp", "tensor"), P("dp", "tensor"), P(None, "tensor")),
        out_specs=(P("dp", "tensor"), P(None, "tensor")),
        check_vma=False,
    )
```

```python
import functools

import jax
import jax.numpy as jnp
from jax import lax
from jax.experimental import pallas as pl
from jax.experimental.pallas import tpu as pltpu
from jax.sharding import PartitionSpec as P


epsilon = 1e-06
tiny = 1e-30
peak = 16384.0
lanes = 128


def pair_weights(low_sq, high_sq, cross):
    low_sq = jnp.maximum(low_sq, 0.0)
    high_sq = jnp.maximum(high_sq, 0.0)
    most = jnp.sqrt(low_sq) * jnp.sqrt(high_sq)
    cross = jnp.minimum(jnp.maximum(cross, -most), most)
    return 1.0 - cross / (2.0 * (low_sq + epsilon)), 1.0 - cross / (2.0 * (high_sq + epsilon))


def merge_coefs(products):
    count = len(products)
    members = [{i: None} for i in range(count)]
    table = products
    while len(table) > 1:
        half = len(table) // 2
        weights = [
            pair_weights(table[2 * i][2 * i], table[2 * i + 1][2 * i + 1], table[2 * i][2 * i + 1])
            for i in range(half)
        ]
        members = [
            {
                r: weights[i][side] if w is None else weights[i][side] * w
                for side in (0, 1)
                for r, w in members[2 * i + side].items()
            }
            for i in range(half)
        ]
        table = [
            [
                sum(
                    weights[i][a] * weights[j][b] * table[min(2 * i + a, 2 * j + b)][max(2 * i + a, 2 * j + b)]
                    for a in (0, 1)
                    for b in (0, 1)
                )
                if j >= i
                else None
                for j in range(half)
            ]
            for i in range(half)
        ]
    return [members[0][r] for r in range(count)]


def own_input_grad(cotangent, projection):
    own_rows = lax.all_to_all(projection, "tensor", split_axis=0, concat_axis=1, tiled=True)
    return lax.dot_general(
        lax.all_gather(cotangent, "tensor", axis=1, tiled=True),
        own_rows,
        (((1,), (1,)), ((), ())),
        preferred_element_type=jnp.float32,
    ).astype(jnp.bfloat16)


def whole_gathers(attention, cotangent, projection):
    n, groups = lax.axis_size("dp"), lax.axis_size("tensor")
    rows = attention.shape[0]
    input_grad = own_input_grad(cotangent, projection)
    acts = lax.all_to_all(attention, "dp", split_axis=1, concat_axis=0, tiled=True)
    acts = lax.all_gather(acts, "tensor", axis=1, tiled=True)
    cots = lax.all_gather(cotangent, "dp", axis=0, tiled=True)
    features, columns = acts.shape[1], cots.shape[1]
    grads = lax.dot_general(
        acts.reshape(n, rows, features),
        cots.reshape(n, rows, columns),
        (((1,), (1,)), ((0,), (0,))),
        preferred_element_type=jnp.float32,
    )
    gram = jnp.stack([jnp.sum(grads * grads[i], (1, 2)) for i in range(n)])
    gram = lax.psum(gram, ("dp", "tensor"))
    coefs = jnp.stack(merge_coefs([[gram[i, j] for j in range(n)] for i in range(n)]))
    bound = jnp.maximum(jnp.sum(jnp.abs(coefs) * jnp.sqrt(jnp.diagonal(gram))), tiny)
    piece = jnp.sum(coefs[:, None, None] * grads, 0)
    sent = (piece * (peak / bound)).astype(jnp.float16)
    gathered = lax.all_gather(sent, "dp", axis=0).astype(jnp.float32) * (bound / peak)
    gathered = gathered.reshape(n, groups, features // groups, columns)
    return (input_grad, gathered.transpose(1, 0, 2, 3).reshape(-1, columns))


def fetch(pairs, sems):
    copies = [pltpu.make_async_copy(source, target, sems.at[i]) for i, (source, target) in enumerate(pairs)]
    for copy in copies:
        copy.start()
    return copies


def grads_kernel(replicas, groups, before, index_ref, *refs):
    slices, refs = refs[:groups], refs[groups:]
    cots, refs = refs[:replicas], refs[replicas:]
    lines = before // replicas
    earlier, refs = refs[:lines], refs[lines:]
    total_ref, refs = (refs[0], refs[1:]) if lines else (None, refs)
    grads_ref, gram_ref, acts, cotangents, held, sems = refs
    width, columns = acts.shape[3], cotangents.shape[2]
    count = index_ref.shape[0] - groups
    features = groups * width
    loads = fetch(
        [(cots[l], cotangents.at[l]) for l in range(replicas)]
        + [(slices[m], acts.at[m]) for m in range(groups)]
        + [(earlier[i], held.at[i]) for i in range(lines)],
        sems,
    )
    for copy in loads[:replicas]:
        copy.wait()
    for m in range(groups):
        loads[replicas + m].wait()
        for l in range(replicas):
            at = pl.multiple_of(index_ref[m] * width, width)
            held[lines, l, pl.ds(at, width), :] = lax.dot_general(
                acts[m, l],
                cotangents[l],
                (((0,), (0,)), ((), ())),
                preferred_element_type=jnp.float32,
            )
    store = pltpu.make_async_copy(held.at[lines], grads_ref, sems.at[len(loads)])
    store.start()
    for copy in loads[groups + replicas :]:
        copy.wait()
    blocks = [(i, l) for i in range(lines + 1) for l in range(replicas)]
    pairs = [(a, b) for b in range(before, before + replicas) for a in range(b + 1)]

    def body(chunk, sums):
        at = pl.multiple_of(chunk * 8, 8)
        values = [held[i, l, pl.ds(at, 8), :] for i, l in blocks]
        fresh = []
        for (a, b), total in zip(pairs, sums):
            product = values[a] * values[b]
            for j in range(columns // lanes):
                total = total + product[:, j * lanes : (j + 1) * lanes]
            fresh.append(total)
        return tuple(fresh)

    zero = jnp.zeros((8, lanes), jnp.float32)
    sums = lax.fori_loop(0, features // 8, body, tuple(zero for _ in pairs))
    col = lax.broadcasted_iota(jnp.int32, (1, lanes), 1)
    gram = total_ref[0] if lines else jnp.zeros((1, lanes), jnp.float32)
    for (a, b), total in zip(pairs, sums):
        value = jnp.sum(jnp.sum(total, axis=0, keepdims=True), axis=1, keepdims=True)
        low = jnp.minimum(index_ref[groups + a], index_ref[groups + b])
        high = jnp.maximum(index_ref[groups + a], index_ref[groups + b])
        gram = gram + jnp.where(col == low * count + high, value, 0.0)
    gram_ref[...] = jnp.broadcast_to(gram[None], gram_ref.shape)
    store.wait()


def combine_kernel(replicas, groups, index_ref, gram_ref, *refs):
    blocks, (piece_ref, scale_ref, held, sems) = refs[:-4], refs[-4:]
    count = len(blocks) * replicas
    features, _ = piece_ref.shape
    chunks = 4
    span = features // chunks
    loads = fetch(
        [
            (block.at[:, pl.ds(c * span, span), :], held.at[i, :, pl.ds(c * span, span), :])
            for c in range(chunks)
            for i, block in enumerate(blocks)
        ],
        sems,
    )
    gram = gram_ref[0]
    for source in range(1, gram_ref.shape[0]):
        gram = gram + gram_ref[source]
    col = lax.broadcasted_iota(jnp.int32, gram.shape, 1)

    def entry(i, j):
        return jnp.sum(jnp.where(col == i * count + j, gram, 0.0), axis=1, keepdims=True)

    products = [[entry(i, j) if j >= i else None for j in range(count)] for i in range(count)]
    coefs = merge_coefs(products)
    bound = sum(jnp.abs(coefs[i]) * jnp.sqrt(products[i][i]) for i in range(count))
    bound = jnp.maximum(bound, tiny)
    scale_ref[...] = bound * (1.0 / peak)
    weights = []
    for at in range(count):
        weight = sum(jnp.where(index_ref[groups + at] == i, coefs[i], 0.0) for i in range(count))
        weights.append(weight * (peak / bound))

    def body(chunk, carry):
        at = pl.multiple_of(chunk * 16, 16)
        total = None
        for block in range(len(blocks)):
            for l in range(replicas):
                term = held[block, l, pl.ds(at, 16), :] * weights[block * replicas + l]
                total = term if total is None else total + term
        piece_ref[pl.ds(at, 16), :] = total
        return carry

    for c in range(chunks):
        for copy in loads[c * len(blocks) : (c + 1) * len(blocks)]:
            copy.wait()
        lax.fori_loop(c * span // 16, (c + 1) * span // 16, body, 0)


def pack_kernel(index_ref, attention_ref, packed_ref):
    packed_ref[...] = attention_ref[...].reshape(packed_ref.shape)


def pack(index, attention, width):
    rows = attention.shape[0]
    return pl.pallas_call(
        pack_kernel,
        grid_spec=pltpu.PrefetchScalarGridSpec(
            num_scalar_prefetch=1,
            grid=(index.shape[0],),
            in_specs=[pl.BlockSpec((rows, width), lambda i, index: (0, index[i]))],
            out_specs=pl.BlockSpec((1, rows, width), lambda i, index: (i, 0, 0)),
        ),
        out_shape=jax.ShapeDtypeStruct((index.shape[0], rows, width), attention.dtype),
        compiler_params=pltpu.CompilerParams(vmem_limit_bytes=4 * 2**20),
        name="pack",
    )(index, attention)


def after(value, *others):
    return lax.optimization_barrier((value, *others))[0]


def unwritten(shape):
    return pl.pallas_call(
        lambda out_ref: None,
        out_shape=jax.ShapeDtypeStruct(shape, jnp.float32),
        out_specs=pl.BlockSpec(memory_space=pltpu.HBM),
        name="unwritten",
    )()


def exchanges(attention, cotangent, projection):
    n, groups = lax.axis_size("dp"), lax.axis_size("tensor")
    inner = 2 ** ((n.bit_length() - 1) // 2)
    outer, pairs = n // inner, groups // 2
    rows, features_here = attention.shape
    columns = cotangent.shape[1]
    width = features_here // n
    features = width * groups
    me, part = lax.axis_index("dp"), lax.axis_index("tensor")
    z, y = me // inner, me % inner
    x, core = part // 2, part % 2

    def along_z(value, place):
        ring = [(i * inner + j, place(i) * inner + j) for i in range(outer) for j in range(inner)]
        return lax.ppermute(value, "dp", ring)

    def along_y(value, l):
        ring = [(i * inner + j, i * inner + (j ^ l)) for i in range(outer) for j in range(inner)]
        return lax.ppermute(value, "dp", ring)

    def along_tensor(value, j, flip):
        ring = [(a * 2 + c, (a + j) % pairs * 2 + (c ^ flip)) for a in range(pairs) for c in range(2)]
        return lax.ppermute(value, "tensor", ring)

    def along_both(found):
        return {k: [found[k]] + [along_y(found[k], l) for l in range(1, inner)] for k in found}

    def by_exchange(value):
        found = {0: value}
        step = outer // 2
        while step:
            for k in list(found):
                found[k ^ step] = along_z(found[k], lambda i: i ^ step)
            step //= 2
        return along_both({k: found[k] for k in range(outer)})

    def by_ring(value):
        found = {0: value, 1: along_z(value, lambda i: (i + 1) % outer)}
        for k in range(2, outer // 2 + 1):
            found[k] = along_z(found[k - 1], lambda i: (i + 1) % outer)
        for k in range(outer - 1, outer // 2, -1):
            found[k] = along_z(found[(k + 1) % outer], lambda i: (i - 1) % outer)
        return along_both({k: found[k] for k in ring_order})

    ring_order = [0, 1] + [k for k in range(outer - 1, outer // 2, -1)] + list(range(2, outer // 2 + 1))

    def replica_of(k, l):
        return (z ^ k) * inner + (y ^ l)

    cots = by_exchange(cotangent)

    own_rows = projection.reshape(groups, -1, columns)

    def rows_for(j, flip):
        target = (x + j) % pairs * 2 + (core ^ flip)
        return lax.dynamic_index_in_dim(own_rows, target, 0, keepdims=False)

    row_blocks = {
        (j, flip): along_tensor(rows_for(j, flip), j, flip) if j or flip else rows_for(0, 0)
        for j in range(pairs)
        for flip in (0, 1)
    }
    cot_blocks = {(j, 0): along_tensor(cotangent, j, 0) if j else cotangent for j in range(pairs)}
    cot_blocks.update({(j, 1): along_tensor(cot_blocks[j, 0], 0, 1) for j in range(pairs)})

    targets = [
        jnp.stack([replica_of(k, l) for k in range(outer)]).astype(jnp.int32)
        for l in range(inner)
    ]
    from_y = [
        along_y(pack(targets[l], attention, width), l) if l else pack(targets[0], attention, width)
        for l in range(inner)
    ]
    slices, slots = {}, []
    for k in range(outer):
        held = jnp.stack([from_y[l][k] for l in range(inner)])
        if k:
            held = along_z(held, lambda i: i ^ k)
        shifted = [held] + [along_tensor(held, j, 0) for j in range(1, pairs)]
        slices[k] = shifted + [along_tensor(value, 0, 1) for value in shifted]
    for flip in (0, 1):
        slots += [(x - j) % pairs * 2 + (core ^ flip) for j in range(pairs)]

    order = [replica_of(k, l) for k in range(outer) for l in range(inner)]
    index = jnp.stack([jnp.asarray(v, jnp.int32) for v in slots + order])
    grads, gram = [], None
    smem, hbm = pl.BlockSpec(memory_space=pltpu.SMEM), pl.BlockSpec(memory_space=pltpu.HBM)
    for at, k in enumerate(range(outer)):
        operands = [*slices[k], *cots[k], *grads]
        vmem = pl.BlockSpec(memory_space=pltpu.VMEM)
        so_far = [gram] if grads else []
        copies = n * groups if k == outer - 1 else 1
        block, gram = pl.pallas_call(
            functools.partial(grads_kernel, inner, groups, at * inner),
            in_specs=[smem] + [hbm] * len(operands) + [vmem] * len(so_far),
            out_specs=(hbm, vmem),
            out_shape=(
                jax.ShapeDtypeStruct((inner, features, columns), jnp.float32),
                jax.ShapeDtypeStruct((copies, 1, lanes), jnp.float32),
            ),
            scratch_shapes=[
                pltpu.VMEM((groups, inner, rows, width), attention.dtype),
                pltpu.VMEM((inner, rows, columns), cotangent.dtype),
                pltpu.VMEM((at + 1, inner, features, columns), jnp.float32),
                pltpu.SemaphoreType.DMA((len(operands) + 1,)),
            ],
            cost_estimate=pl.CostEstimate(
                flops=2 * inner * rows * features * columns,
                bytes_accessed=8 * inner * features * columns,
                transcendentals=0,
            ),
        )(index, *operands, *so_far)
        grads.append(block)

    shared = lax.all_to_all(gram, ("dp", "tensor"), 0, 0, tiled=True).reshape(n * groups, 1, lanes)
    sent, scale = pl.pallas_call(
        functools.partial(combine_kernel, inner, groups),
        in_specs=[smem, pl.BlockSpec(memory_space=pltpu.VMEM)] + [hbm] * outer,
        out_specs=(pl.BlockSpec(memory_space=pltpu.VMEM), pl.BlockSpec(memory_space=pltpu.VMEM)),
        out_shape=(
            jax.ShapeDtypeStruct((features, columns), jnp.float32),
            jax.ShapeDtypeStruct((1, 1), jnp.float32),
        ),
        scratch_shapes=[
            pltpu.VMEM((outer, inner, features, columns), jnp.float32),
            pltpu.SemaphoreType.DMA((4 * outer,)),
        ],
        cost_estimate=pl.CostEstimate(
            flops=2 * n * features * columns, bytes_accessed=4 * n * features * columns, transcendentals=0
        ),
        name="combine",
    )(index, shared, *grads)
    combined = unwritten((groups, n, width, columns))
    lines = by_ring(after(sent.astype(jnp.float16)))
    for l in range(inner):
        for k in ring_order:
            values = lines[k][l].reshape(groups, 1, width, columns).astype(jnp.float32) * scale[0, 0]
            source = (z - k) % outer * inner + (y ^ l)
            combined = lax.dynamic_update_slice_in_dim(combined, values, source, 1)
    combined = combined.reshape(groups * n * width, columns)

    total = None
    for key in [(0, 0), (0, 1)] + [(j, flip) for j in range(1, pairs) for flip in (0, 1)]:
        theirs = cot_blocks[key]
        if key != (0, 0):
            theirs = after(theirs, lines[ring_order[2] if key[0] else 1][0])
        term = lax.dot_general(theirs, row_blocks[key], (((1,), (1,)), ((), ())), preferred_element_type=jnp.float32)
        total = term if total is None else total + term
    return (total.astype(jnp.bfloat16), combined)


def on_device(attention, cotangent, projection):
    n, groups = lax.axis_size("dp"), lax.axis_size("tensor")
    aligned = (attention.shape[1] // n) % lanes == 0 and cotangent.shape[1] % lanes == 0
    if aligned and groups % 2 == 0 and 4 <= n <= 8:
        return exchanges(attention, cotangent, projection)
    return whole_gathers(attention, cotangent, projection)


def solution(mesh):
    return jax.shard_map(
        on_device,
        mesh=mesh,
        in_specs=(P("dp", "tensor"), P("dp", "tensor"), P(None, "tensor")),
        out_specs=(P("dp", "tensor"), P(None, "tensor")),
        check_vma=False,
    )
```

```python
import functools

import jax
import jax.numpy as jnp
from jax import lax
from jax.experimental import pallas as pl
from jax.experimental.pallas import tpu as pltpu
from jax.sharding import PartitionSpec as P


epsilon = 1e-06
tiny = 1e-30
peak = 16384.0
lanes = 128


def pair_weights(low_sq, high_sq, cross):
    low_sq = jnp.maximum(low_sq, 0.0)
    high_sq = jnp.maximum(high_sq, 0.0)
    most = jnp.sqrt(low_sq) * jnp.sqrt(high_sq)
    cross = jnp.minimum(jnp.maximum(cross, -most), most)
    return 1.0 - cross / (2.0 * (low_sq + epsilon)), 1.0 - cross / (2.0 * (high_sq + epsilon))


def merge_coefs(products):
    count = len(products)
    members = [{i: None} for i in range(count)]
    table = products
    while len(table) > 1:
        half = len(table) // 2
        weights = [
            pair_weights(table[2 * i][2 * i], table[2 * i + 1][2 * i + 1], table[2 * i][2 * i + 1])
            for i in range(half)
        ]
        members = [
            {
                r: weights[i][side] if w is None else weights[i][side] * w
                for side in (0, 1)
                for r, w in members[2 * i + side].items()
            }
            for i in range(half)
        ]
        table = [
            [
                sum(
                    weights[i][a] * weights[j][b] * table[min(2 * i + a, 2 * j + b)][max(2 * i + a, 2 * j + b)]
                    for a in (0, 1)
                    for b in (0, 1)
                )
                if j >= i
                else None
                for j in range(half)
            ]
            for i in range(half)
        ]
    return [members[0][r] for r in range(count)]


def own_input_grad(cotangent, projection):
    own_rows = lax.all_to_all(projection, "tensor", split_axis=0, concat_axis=1, tiled=True)
    return lax.dot_general(
        lax.all_gather(cotangent, "tensor", axis=1, tiled=True),
        own_rows,
        (((1,), (1,)), ((), ())),
        preferred_element_type=jnp.float32,
    ).astype(jnp.bfloat16)


def whole_gathers(attention, cotangent, projection):
    n, groups = lax.axis_size("dp"), lax.axis_size("tensor")
    rows = attention.shape[0]
    input_grad = own_input_grad(cotangent, projection)
    acts = lax.all_to_all(attention, "dp", split_axis=1, concat_axis=0, tiled=True)
    acts = lax.all_gather(acts, "tensor", axis=1, tiled=True)
    cots = lax.all_gather(cotangent, "dp", axis=0, tiled=True)
    features, columns = acts.shape[1], cots.shape[1]
    grads = lax.dot_general(
        acts.reshape(n, rows, features),
        cots.reshape(n, rows, columns),
        (((1,), (1,)), ((0,), (0,))),
        preferred_element_type=jnp.float32,
    )
    gram = jnp.stack([jnp.sum(grads * grads[i], (1, 2)) for i in range(n)])
    gram = lax.psum(gram, ("dp", "tensor"))
    coefs = jnp.stack(merge_coefs([[gram[i, j] for j in range(n)] for i in range(n)]))
    bound = jnp.maximum(jnp.sum(jnp.abs(coefs) * jnp.sqrt(jnp.diagonal(gram))), tiny)
    piece = jnp.sum(coefs[:, None, None] * grads, 0)
    sent = (piece * (peak / bound)).astype(jnp.float16)
    gathered = lax.all_gather(sent, "dp", axis=0).astype(jnp.float32) * (bound / peak)
    gathered = gathered.reshape(n, groups, features // groups, columns)
    return (input_grad, gathered.transpose(1, 0, 2, 3).reshape(-1, columns))


def fetch(pairs, sems):
    copies = [pltpu.make_async_copy(source, target, sems.at[i]) for i, (source, target) in enumerate(pairs)]
    for copy in copies:
        copy.start()
    return copies


def grads_kernel(replicas, groups, before, index_ref, *refs):
    slices, refs = refs[:groups], refs[groups:]
    cots, refs = refs[:replicas], refs[replicas:]
    lines = before // replicas
    earlier, refs = refs[:lines], refs[lines:]
    total_ref, refs = (refs[0], refs[1:]) if lines else (None, refs)
    grads_ref, gram_ref, acts, cotangents, held, sems = refs
    width, columns = acts.shape[1] // groups, cotangents.shape[2]
    count = index_ref.shape[0] - groups
    features = groups * width
    loads = fetch(
        [(cots[l], cotangents.at[l]) for l in range(replicas)]
        + [(slices[m], acts.at[:, pl.ds(m * width, width), :]) for m in range(groups)]
        + [(earlier[i], held.at[i]) for i in range(lines)],
        sems,
    )
    for copy in loads[: replicas + groups]:
        copy.wait()
    for l in range(replicas):
        block = lax.dot_general(
            acts[l], cotangents[l], (((1,), (0,)), ((), ())), preferred_element_type=jnp.float32
        )
        for m in range(groups):
            at = pl.multiple_of(index_ref[m] * width, width)
            held[lines, l, pl.ds(at, width), :] = block[m * width : (m + 1) * width]
    store = pltpu.make_async_copy(held.at[lines], grads_ref, sems.at[len(loads)])
    store.start()
    for copy in loads[groups + replicas :]:
        copy.wait()
    blocks = [(i, l) for i in range(lines + 1) for l in range(replicas)]
    pairs = [(a, b) for b in range(before, before + replicas) for a in range(b + 1)]

    def body(chunk, sums):
        at = pl.multiple_of(chunk * 8, 8)
        values = [held[i, l, pl.ds(at, 8), :] for i, l in blocks]
        fresh = []
        for (a, b), total in zip(pairs, sums):
            product = values[a] * values[b]
            for j in range(columns // lanes):
                total = total + product[:, j * lanes : (j + 1) * lanes]
            fresh.append(total)
        return tuple(fresh)

    zero = jnp.zeros((8, lanes), jnp.float32)
    sums = lax.fori_loop(0, features // 8, body, tuple(zero for _ in pairs))
    col = lax.broadcasted_iota(jnp.int32, (1, lanes), 1)
    gram = total_ref[0] if lines else jnp.zeros((1, lanes), jnp.float32)
    for (a, b), total in zip(pairs, sums):
        value = jnp.sum(jnp.sum(total, axis=0, keepdims=True), axis=1, keepdims=True)
        low = jnp.minimum(index_ref[groups + a], index_ref[groups + b])
        high = jnp.maximum(index_ref[groups + a], index_ref[groups + b])
        gram = gram + jnp.where(col == low * count + high, value, 0.0)
    gram_ref[...] = jnp.broadcast_to(gram[None], gram_ref.shape)
    store.wait()


def combine_kernel(replicas, groups, index_ref, gram_ref, *refs):
    blocks, (piece_ref, scale_ref, held, sems) = refs[:-4], refs[-4:]
    count = len(blocks) * replicas
    features, _ = piece_ref.shape
    chunks = 4
    span = features // chunks
    loads = fetch(
        [
            (block.at[:, pl.ds(c * span, span), :], held.at[i, :, pl.ds(c * span, span), :])
            for c in range(chunks)
            for i, block in enumerate(blocks)
        ],
        sems,
    )
    gram = gram_ref[0]
    for source in range(1, gram_ref.shape[0]):
        gram = gram + gram_ref[source]
    col = lax.broadcasted_iota(jnp.int32, gram.shape, 1)

    def entry(i, j):
        return jnp.sum(jnp.where(col == i * count + j, gram, 0.0), axis=1, keepdims=True)

    products = [[entry(i, j) if j >= i else None for j in range(count)] for i in range(count)]
    coefs = merge_coefs(products)
    bound = sum(jnp.abs(coefs[i]) * jnp.sqrt(products[i][i]) for i in range(count))
    bound = jnp.maximum(bound, tiny)
    scale_ref[...] = bound * (1.0 / peak)
    weights = []
    for at in range(count):
        weight = sum(jnp.where(index_ref[groups + at] == i, coefs[i], 0.0) for i in range(count))
        weights.append(weight * (peak / bound))

    def body(chunk, carry):
        at = pl.multiple_of(chunk * 16, 16)
        total = None
        for block in range(len(blocks)):
            for l in range(replicas):
                term = held[block, l, pl.ds(at, 16), :] * weights[block * replicas + l]
                total = term if total is None else total + term
        piece_ref[pl.ds(at, 16), :] = total
        return carry

    for c in range(chunks):
        for copy in loads[c * len(blocks) : (c + 1) * len(blocks)]:
            copy.wait()
        lax.fori_loop(c * span // 16, (c + 1) * span // 16, body, 0)


def pack_kernel(index_ref, attention_ref, packed_ref):
    packed_ref[0] = attention_ref[...].T


def pack(index, attention, width):
    rows = attention.shape[0]
    return pl.pallas_call(
        pack_kernel,
        grid_spec=pltpu.PrefetchScalarGridSpec(
            num_scalar_prefetch=1,
            grid=(index.shape[0],),
            in_specs=[pl.BlockSpec((rows, width), lambda i, index: (0, index[i]))],
            out_specs=pl.BlockSpec((1, width, rows), lambda i, index: (i, 0, 0)),
        ),
        out_shape=jax.ShapeDtypeStruct((index.shape[0], width, rows), attention.dtype),
        compiler_params=pltpu.CompilerParams(vmem_limit_bytes=4 * 2**20),
        name="pack",
    )(index, attention)


def after(value, *others):
    return lax.optimization_barrier((value, *others))[0]


def unwritten(shape):
    return pl.pallas_call(
        lambda out_ref: None,
        out_shape=jax.ShapeDtypeStruct(shape, jnp.float32),
        out_specs=pl.BlockSpec(memory_space=pltpu.HBM),
        name="unwritten",
    )()


def exchanges(attention, cotangent, projection):
    n, groups = lax.axis_size("dp"), lax.axis_size("tensor")
    inner = 2 ** ((n.bit_length() - 1) // 2)
    outer, pairs = n // inner, groups // 2
    rows, features_here = attention.shape
    columns = cotangent.shape[1]
    width = features_here // n
    features = width * groups
    me, part = lax.axis_index("dp"), lax.axis_index("tensor")
    z, y = me // inner, me % inner
    x, core = part // 2, part % 2

    def along_z(value, place):
        ring = [(i * inner + j, place(i) * inner + j) for i in range(outer) for j in range(inner)]
        return lax.ppermute(value, "dp", ring)

    def along_y(value, l):
        ring = [(i * inner + j, i * inner + (j ^ l)) for i in range(outer) for j in range(inner)]
        return lax.ppermute(value, "dp", ring)

    def along_tensor(value, j, flip):
        ring = [(a * 2 + c, (a + j) % pairs * 2 + (c ^ flip)) for a in range(pairs) for c in range(2)]
        return lax.ppermute(value, "tensor", ring)

    def along_both(found):
        return {k: [found[k]] + [along_y(found[k], l) for l in range(1, inner)] for k in found}

    def by_exchange(value):
        found = {0: value}
        step = outer // 2
        while step:
            for k in list(found):
                found[k ^ step] = along_z(found[k], lambda i: i ^ step)
            step //= 2
        return along_both({k: found[k] for k in range(outer)})

    def by_ring(value):
        found = {0: value, 1: along_z(value, lambda i: (i + 1) % outer)}
        for k in range(2, outer // 2 + 1):
            found[k] = along_z(found[k - 1], lambda i: (i + 1) % outer)
        for k in range(outer - 1, outer // 2, -1):
            found[k] = along_z(found[(k + 1) % outer], lambda i: (i - 1) % outer)
        return along_both({k: found[k] for k in ring_order})

    ring_order = [0, 1] + [k for k in range(outer - 1, outer // 2, -1)] + list(range(2, outer // 2 + 1))

    def replica_of(k, l):
        return (z ^ k) * inner + (y ^ l)

    cots = by_exchange(cotangent)

    own_rows = projection.reshape(groups, -1, columns)

    def rows_for(j, flip):
        target = (x + j) % pairs * 2 + (core ^ flip)
        return lax.dynamic_index_in_dim(own_rows, target, 0, keepdims=False)

    row_blocks = {
        (j, flip): along_tensor(rows_for(j, flip), j, flip) if j or flip else rows_for(0, 0)
        for j in range(pairs)
        for flip in (0, 1)
    }
    cot_blocks = {(j, 0): along_tensor(cotangent, j, 0) if j else cotangent for j in range(pairs)}
    cot_blocks.update({(j, 1): along_tensor(cot_blocks[j, 0], 0, 1) for j in range(pairs)})

    targets = [
        jnp.stack([replica_of(k, l) for k in range(outer)]).astype(jnp.int32)
        for l in range(inner)
    ]
    from_y = [
        along_y(pack(targets[l], attention, width), l) if l else pack(targets[0], attention, width)
        for l in range(inner)
    ]
    slices, slots = {}, []
    for k in range(outer):
        held = jnp.stack([from_y[l][k] for l in range(inner)])
        if k:
            held = along_z(held, lambda i: i ^ k)
        shifted = [held] + [along_tensor(held, j, 0) for j in range(1, pairs)]
        slices[k] = shifted + [along_tensor(value, 0, 1) for value in shifted]
    for flip in (0, 1):
        slots += [(x - j) % pairs * 2 + (core ^ flip) for j in range(pairs)]

    order = [replica_of(k, l) for k in range(outer) for l in range(inner)]
    index = jnp.stack([jnp.asarray(v, jnp.int32) for v in slots + order])
    grads, gram = [], None
    smem, hbm = pl.BlockSpec(memory_space=pltpu.SMEM), pl.BlockSpec(memory_space=pltpu.HBM)
    for at, k in enumerate(range(outer)):
        operands = [*slices[k], *cots[k], *grads]
        vmem = pl.BlockSpec(memory_space=pltpu.VMEM)
        so_far = [gram] if grads else []
        copies = n * groups if k == outer - 1 else 1
        block, gram = pl.pallas_call(
            functools.partial(grads_kernel, inner, groups, at * inner),
            in_specs=[smem] + [hbm] * len(operands) + [vmem] * len(so_far),
            out_specs=(hbm, vmem),
            out_shape=(
                jax.ShapeDtypeStruct((inner, features, columns), jnp.float32),
                jax.ShapeDtypeStruct((copies, 1, lanes), jnp.float32),
            ),
            scratch_shapes=[
                pltpu.VMEM((inner, features, rows), attention.dtype),
                pltpu.VMEM((inner, rows, columns), cotangent.dtype),
                pltpu.VMEM((at + 1, inner, features, columns), jnp.float32),
                pltpu.SemaphoreType.DMA((len(operands) + 1,)),
            ],
            cost_estimate=pl.CostEstimate(
                flops=2 * inner * rows * features * columns,
                bytes_accessed=8 * inner * features * columns,
                transcendentals=0,
            ),
        )(index, *operands, *so_far)
        grads.append(block)

    shared = lax.all_to_all(gram, ("dp", "tensor"), 0, 0, tiled=True).reshape(n * groups, 1, lanes)

    def input_term(key, *others):
        return lax.dot_general(
            after(cot_blocks[key], *others),
            row_blocks[key],
            (((1,), (1,)), ((), ())),
            preferred_element_type=jnp.float32,
        )

    total = input_term((0, 0), gram) + input_term((0, 1), gram)
    shared = after(shared, total)
    sent, scale = pl.pallas_call(
        functools.partial(combine_kernel, inner, groups),
        in_specs=[smem, pl.BlockSpec(memory_space=pltpu.VMEM)] + [hbm] * outer,
        out_specs=(pl.BlockSpec(memory_space=pltpu.VMEM), pl.BlockSpec(memory_space=pltpu.VMEM)),
        out_shape=(
            jax.ShapeDtypeStruct((features, columns), jnp.float32),
            jax.ShapeDtypeStruct((1, 1), jnp.float32),
        ),
        scratch_shapes=[
            pltpu.VMEM((outer, inner, features, columns), jnp.float32),
            pltpu.SemaphoreType.DMA((4 * outer,)),
        ],
        cost_estimate=pl.CostEstimate(
            flops=2 * n * features * columns, bytes_accessed=4 * n * features * columns, transcendentals=0
        ),
        name="combine",
    )(index, shared, *grads)
    combined = unwritten((groups, n, width, columns))
    lines = by_ring(after(sent.astype(jnp.float16)))
    half = outer // 2
    for l in range(1, inner):
        first, second = lines[half][0][: features // 2], lines[half - 1][l][features // 2 :]
        lines[half][l] = [along_y(first, l), along_z(second, lambda i: (i + 1) % outer)]
    for k in ring_order:
        for l in range(inner):
            source = (z - k) % outer * inner + (y ^ l)
            parts = lines[k][l] if isinstance(lines[k][l], list) else [lines[k][l]]
            for at, block in enumerate(parts):
                share = groups // len(parts)
                values = block.reshape(share, 1, width, columns).astype(jnp.float32) * scale[0, 0]
                combined = lax.dynamic_update_slice(combined, values, (at * share, source, 0, 0))
    combined = combined.reshape(groups * n * width, columns)

    for key in [(j, flip) for j in range(1, pairs) for flip in (0, 1)]:
        total = total + input_term(key, lines[ring_order[2]][0])
    return (total.astype(jnp.bfloat16), combined)


def on_device(attention, cotangent, projection):
    n, groups = lax.axis_size("dp"), lax.axis_size("tensor")
    aligned = (attention.shape[1] // n) % lanes == 0 and cotangent.shape[1] % lanes == 0
    if aligned and groups % 2 == 0 and 4 <= n <= 8:
        return exchanges(attention, cotangent, projection)
    return whole_gathers(attention, cotangent, projection)


def solution(mesh):
    return jax.shard_map(
        on_device,
        mesh=mesh,
        in_specs=(P("dp", "tensor"), P("dp", "tensor"), P(None, "tensor")),
        out_specs=(P("dp", "tensor"), P(None, "tensor")),
        check_vma=False,
    )
```
